32 devices in a mesh: gx: 4 (over z), gy: 8 (over y, x, core).
Axes of the slice: x: 2, y: 2, z: 4, core: 2. Of those that a mesh axis runs over, the one named last changes fastest.
Arguments:
- tables: float32 [2, 262144, 128], P(None, ('gx', 'gy')), may hold values from -0.9 to 0.9
- cold_rows: int32 [32, 2, 32, 16], P(('gx', 'gy')), may hold values from 0 to 8191, as said below
- cold_bags: int32 [32, 2, 32, 16], P(('gx', 'gy')), may hold values from -1 to 127, as said below
- hot_rows: int32 [2, 256], replicated, may hold values from 0 to 262143
- hot_ids: int32 [4096, 2, 8], P(('gx', 'gy')), may hold values from 0 to 255
Outputs:
- pooled: float32 [4096, 2, 128], P(('gx', 'gy'))
The draws below stay inside these ranges and needn't reach their ends.
Inputs may be any that keep to these rules, and one draw needn't show every extreme that they name: `cold_rows`: every entry names one of the owner's 8192 rows. `cold_bags`: live slots of one sender, table and owner come first, the empty ones (-1) after them; in every draw each table has an owner whose 16 slots are all live from every sender.
All inputs are finite; a program needn't handle non-finite values.
Results may differ from the reference program's by a relative error of at most 0.0003.
Values sent between devices are 32-bit elements; how exact they have to be, the bound alone decides.
A program may use at most 64 MiB of HBM per device.

```python
import jax
import jax.numpy as jnp
from jax import lax

DIM = 128
ROWS_DEV = 8192
TABLES = 2
BATCH_DEV = 128
CAP = 16
HOT = 256
HOT_BAG = 8
PEERS = 32
BATCH = 4096
ROWS = 262144


def draw_cold_rows(key, part):
    shape_all = (PEERS, TABLES, PEERS, CAP)
    exponent = jax.random.randint(jax.random.fold_in(key, 101), shape_all, 0, 21)
    limit = jnp.minimum(jnp.left_shift(jnp.ones(shape_all, jnp.int32), exponent), ROWS_DEV)
    return jax.random.randint(jax.random.fold_in(key, 102), shape_all, 0, limit).astype(jnp.int32)


def draw_cold_bags(key, part):
    shape_all = (PEERS, TABLES, PEERS, CAP)
    busiest = jax.random.randint(jax.random.fold_in(key, 201), (TABLES,), 0, PEERS)
    filled = jax.random.randint(jax.random.fold_in(key, 202), (PEERS, TABLES, PEERS), max(1, CAP // 4), CAP + 1)
    owner_index = jnp.arange(PEERS, dtype=jnp.int32)[None, None, :]
    filled = jnp.where(owner_index == busiest[None, :, None], CAP, filled)
    samples = jax.random.randint(jax.random.fold_in(key, 203), shape_all, 0, BATCH_DEV)
    slot_index = jnp.arange(CAP, dtype=jnp.int32)
    return jnp.where(slot_index < filled[..., None], samples, -1).astype(jnp.int32)


def place_ends(entries, rng, smallest, largest):
    longest = entries.shape.index(max(entries.shape))
    spots = []
    for shift in (0, 1):
        where = [jax.random.randint(jax.random.fold_in(rng, axis), (), 0, length) for axis, length in enumerate(entries.shape)]
        where[longest] = (where[longest] + shift) % entries.shape[longest]
        spots.append(tuple(where))
    return entries.at[spots[0]].set(smallest).at[spots[1]].set(largest)


def shard_levels(own_key, extent, pieces, least, high):
    def one(position, parts):
        draws = jax.random.uniform(jax.random.fold_in(jax.random.fold_in(own_key, 6), position), (parts,), jnp.float32, least / len(pieces), high / len(pieces))
        return jnp.repeat(jnp.exp(draws), extent[position] // parts).reshape((-1,) + (1,) * (len(extent) - position - 1))

    gain = one(*pieces[0])
    for cut in pieces[1:]:
        gain = gain * one(*cut)
    return gain


def centred(stream_key, shape, deviation, reach, cuts=(), kind=jnp.bfloat16):
    drawn = jax.random.normal(stream_key, shape, jnp.float32) * deviation
    if len(cuts) > 0:
        drawn = shard_levels(stream_key, shape, cuts, -0.22, 0.18) * drawn
    return jnp.clip(drawn, min=-reach, max=reach).astype(kind)


def setup_inputs(seed: int = 0) -> dict:
    key_list = jax.random.split(jax.random.key(seed), 6)
    return {
        "tables": centred(key_list[0], (TABLES, ROWS, DIM), 0.15, 0.9, ((1, 32),), jnp.float32),
        "cold_rows": draw_cold_rows(jax.random.fold_in(key_list[5], 71), 0),
        "cold_bags": draw_cold_bags(jax.random.fold_in(key_list[5], 71), 0),
        "hot_rows": place_ends(jax.random.randint(key_list[3], (TABLES, HOT), 0, ROWS), jax.random.fold_in(key_list[3], 1), 0, ROWS - 1).astype(jnp.int32),
        "hot_ids": place_ends(jax.random.randint(key_list[4], (BATCH, TABLES, HOT_BAG), 0, HOT), jax.random.fold_in(key_list[4], 1), 0, HOT - 1).astype(jnp.int32),
    }


def take_rows(matrix, indices):
    return jnp.take(matrix, indices, axis=0)


def reference(tables, cold_rows, cold_bags, hot_rows, hot_ids):
    offsets = (jnp.arange(PEERS, dtype=jnp.int32) * ROWS_DEV)[:, None]

    def per_table(table_index):
        one_table = tables[table_index]

        def per_sender(sender):
            slot_rows = (cold_rows[sender, table_index] + offsets).reshape(-1)
            slot_bags = cold_bags[sender, table_index].reshape(-1)
            looked = take_rows(one_table, slot_rows)
            live_mask = slot_bags >= 0
            segment = jnp.where(live_mask, slot_bags, 0).astype(jnp.int32)
            values = jnp.where(live_mask[:, None], looked, jnp.zeros_like(looked))
            return jax.ops.segment_sum(values, segment, num_segments=BATCH_DEV)

        return lax.map(per_sender, jnp.arange(PEERS, dtype=jnp.int32))

    cold_part = lax.map(per_table, jnp.arange(TABLES, dtype=jnp.int32))
    cold_part = jnp.transpose(cold_part, (1, 2, 0, 3)).reshape(BATCH, TABLES, DIM)
    hot_table = jax.vmap(take_rows)(tables, hot_rows)

    def pool_hot(table_rows, lookups):
        return jnp.sum(take_rows(table_rows, lookups), axis=1)

    hot_part = jax.vmap(pool_hot, in_axes=(0, 1), out_axes=1)(hot_table, hot_ids)
    return cold_part + hot_part
```

```python
import functools

import jax
import jax.numpy as jnp
from jax import lax
from jax.experimental import pallas as pl
from jax.experimental.pallas import tpu as pltpu
from jax.sharding import PartitionSpec as P

MESH = pl.DeviceIdType.MESH
CHUNKS = 4


def split2(x):
    hi = x.astype(jnp.bfloat16)
    return hi, (x - hi.astype(jnp.float32)).astype(jnp.bfloat16)


def pool(weights, values):
    hi, lo = split2(values)
    return jnp.dot(weights, hi, preferred_element_type=jnp.float32) + jnp.dot(
        weights, lo, preferred_element_type=jnp.float32
    )


def kernel(nx, ny, tables_ref, rows_ref, bags_ref, hot_rows_ref, hot_ids_ref, out_ref,
           tab, idx_out, idx_in, idx_s, stage, recv, hot_stage, hot_in, hot_tab, onehot, counts,
           tab_sem, idx_send, idx_recv, idx_local, cold_send, cold_recv,
           hot_send, hot_recv, gat_send, gat_recv):
    peers = nx * ny
    tcount, rows_dev, width = tab.shape
    cap = rows_ref.shape[3]
    hot = hot_rows_ref.shape[1]
    share = hot_tab.shape[0] // peers
    batch = out_ref.shape[0]
    gx, gy = lax.axis_index("gx"), lax.axis_index("gy")
    me = gx * ny + gy

    def peer(i):
        px = lax.rem(gx + lax.rem(i, nx) + nx // 2, nx)
        py = lax.rem(gy + i // nx, ny)
        return px, py, px * ny + py

    self_at = (nx - nx // 2) % nx

    def others(fn):
        def step(i, carry):
            @pl.when(i != self_at)
            def _():
                fn(*peer(i))
            return carry
        lax.fori_loop(0, peers, step, 0)

    piece = rows_dev // CHUNKS
    loads = []
    for t in range(tcount):
        for c in range(CHUNKS):
            part = pl.ds(c * piece, piece)
            load = pltpu.make_async_copy(tables_ref.at[t, part], tab.at[t, part], tab_sem.at[t, c])
            load.start()
            loads.append(load)

    barrier = pltpu.get_barrier_semaphore()
    others(lambda px, py, p: pl.semaphore_signal(
        barrier, inc=1, device_id=(px, py), device_id_type=MESH))

    for p in range(peers):
        for t in range(tcount):
            idx_out[p, :, t * cap:(t + 1) * cap] = rows_ref[0, t, p:p + 1, :]
    idx_in[me] = idx_out[me]
    pl.semaphore_wait(barrier, peers - 1)

    def send_idx(px, py, p):
        pltpu.make_async_remote_copy(
            src_ref=idx_out.at[p], dst_ref=idx_in.at[me], send_sem=idx_send, recv_sem=idx_recv,
            device_id=(px, py), device_id_type=MESH).start()
    others(send_idx)

    for load in loads:
        load.wait()

    base = me * rows_dev

    def pick_hot(p):
        start = p * share
        t = start // hot
        first = start - t * hot
        for j in range(share):
            local = hot_rows_ref[t, first + j] - base
            mine = jnp.logical_and(local >= 0, local < rows_dev).astype(jnp.float32)
            at = jnp.clip(local, 0, rows_dev - 1)
            hot_stage[p, j:j + 1, :] = tab[t, pl.ds(at, 1), :] * mine

    def all_hot(p, carry):
        pick_hot(p)
        return carry
    lax.fori_loop(0, peers, all_hot, 0)

    def send_hot(px, py, p):
        pltpu.make_async_remote_copy(
            src_ref=hot_stage.at[p], dst_ref=hot_in.at[me], send_sem=hot_send, recv_sem=hot_recv,
            device_id=(px, py), device_id_type=MESH).start()
    others(send_hot)
    hot_in[me] = hot_stage[me]

    some = pl.ds(0, peers - 1)
    pltpu.make_async_copy(idx_in.at[some], idx_in.at[some], idx_recv).wait()
    to_smem = pltpu.make_async_copy(idx_in, idx_s, idx_local)
    to_smem.start()
    to_smem.wait()

    def pick(p):
        for t in range(tcount):
            for c in range(cap):
                k = t * cap + c
                stage[p, k:k + 1, :] = tab[t, pl.ds(idx_s[p, 0, k], 1), :]

    def send_cold(px, py, p):
        pltpu.make_async_remote_copy(
            src_ref=stage.at[p], dst_ref=recv.at[me], send_sem=cold_send, recv_sem=cold_recv,
            device_id=(px, py), device_id_type=MESH).start()

    def cold_step(i, carry):
        @pl.when(i < peers)
        def _():
            pick(peer(i)[2])

        @pl.when(jnp.logical_and(i > 0, i - 1 != self_at))
        def _():
            send_cold(*peer(i - 1))
        return carry
    lax.fori_loop(0, peers + 1, cold_step, 0)
    recv[me] = stage[me]

    pltpu.make_async_copy(hot_in.at[some], hot_in.at[some], hot_recv).wait()
    mine_at = pl.ds(pl.multiple_of(me * share, share), share)
    hot_tab[mine_at, :] = jnp.sum(hot_in[...], axis=0)

    slots = peers * cap
    col = lax.broadcasted_iota(jnp.int32, (cap, slots), 1)
    spread = (lax.rem(col, cap) == lax.broadcasted_iota(jnp.int32, (cap, slots), 0)).astype(jnp.float32)
    owner = lax.broadcasted_iota(jnp.int32, (peers, slots), 1) // cap
    mask = owner == lax.broadcasted_iota(jnp.int32, (peers, slots), 0)
    samples = lax.broadcasted_iota(jnp.int32, (batch, slots), 0).astype(jnp.float32)
    for t in range(tcount):
        wide = jnp.dot(bags_ref[0, t].astype(jnp.float32), spread,
                       precision=lax.Precision.HIGHEST, preferred_element_type=jnp.float32)
        flat = jnp.sum(jnp.where(mask, wide, 0.0), axis=0, keepdims=True)
        onehot[t] = (flat == samples).astype(jnp.bfloat16)

    def send_gat(px, py, p):
        pltpu.make_async_remote_copy(
            src_ref=hot_tab.at[mine_at], dst_ref=hot_tab.at[mine_at], send_sem=gat_send,
            recv_sem=gat_recv, device_id=(px, py), device_id_type=MESH).start()
    others(send_gat)

    ids_count = hot_ids_ref.shape[1] // tcount
    entry = lax.broadcasted_iota(jnp.int32, (batch, hot), 1)
    ids = hot_ids_ref[...]
    for t in range(tcount):
        total = jnp.zeros((batch, hot), jnp.float32)
        for k in range(ids_count):
            c = t * ids_count + k
            total += (ids[:, c:c + 1] == entry).astype(jnp.float32)
        counts[t] = total.astype(jnp.bfloat16)

    pltpu.make_async_copy(recv.at[some], recv.at[some], cold_recv).wait()
    for t in range(tcount):
        got = recv[:, t * cap:(t + 1) * cap, :].reshape(slots, width)
        out_ref[:, t * width:(t + 1) * width] = pool(onehot[t], got)
    rest = pl.ds(0, (peers - 1) * share)
    pltpu.make_async_copy(hot_tab.at[rest], hot_tab.at[rest], gat_recv).wait()
    for t in range(tcount):
        out_ref[:, t * width:(t + 1) * width] += pool(counts[t], hot_tab[t * hot:(t + 1) * hot, :])

    pltpu.make_async_copy(idx_out.at[some], idx_out.at[some], idx_send).wait()
    pltpu.make_async_copy(hot_stage.at[some], hot_stage.at[some], hot_send).wait()
    pltpu.make_async_copy(stage.at[some], stage.at[some], cold_send).wait()
    pltpu.make_async_copy(hot_tab.at[rest], hot_tab.at[rest], gat_send).wait()


def solution(mesh):
    nx, ny = mesh.shape["gx"], mesh.shape["gy"]
    peers = nx * ny

    def body(tables, cold_rows, cold_bags, hot_rows, hot_ids):
        tcount, rows_dev, width = tables.shape
        cap = cold_rows.shape[3]
        batch = hot_ids.shape[0]
        hot = hot_rows.shape[1]
        share = tcount * hot // peers
        assert share * peers == tcount * hot and hot % share == 0
        lanes = -(-tcount * cap // 128) * 128
        vmem = pl.BlockSpec(memory_space=pltpu.VMEM)
        out = pl.pallas_call(
            functools.partial(kernel, nx, ny),
            out_shape=jax.ShapeDtypeStruct((batch, tcount * width), jnp.float32),
            in_specs=[
                pl.BlockSpec(memory_space=pl.ANY), vmem, vmem,
                pl.BlockSpec(memory_space=pltpu.SMEM), vmem,
            ],
            out_specs=vmem,
            scratch_shapes=[
                pltpu.VMEM((tcount, rows_dev, width), jnp.float32),
                pltpu.VMEM((peers, 1, lanes), jnp.int32),
                pltpu.VMEM((peers, 1, lanes), jnp.int32),
                pltpu.SMEM((peers, 1, lanes), jnp.int32),
                pltpu.VMEM((peers, tcount * cap, width), jnp.float32),
                pltpu.VMEM((peers, tcount * cap, width), jnp.float32),
                pltpu.VMEM((peers, share, width), jnp.float32),
                pltpu.VMEM((peers, share, width), jnp.float32),
                pltpu.VMEM((tcount * hot, width), jnp.float32),
                pltpu.VMEM((tcount, batch, peers * cap), jnp.bfloat16),
                pltpu.VMEM((tcount, batch, hot), jnp.bfloat16),
                pltpu.SemaphoreType.DMA((tcount, CHUNKS)),
            ] + [pltpu.SemaphoreType.DMA] * 9,
            compiler_params=pltpu.CompilerParams(
                collective_id=0, has_side_effects=True, vmem_limit_bytes=48 * 1024 * 1024),
        )(tables, cold_rows, cold_bags, hot_rows, hot_ids.reshape(batch, -1))
        return out.reshape(batch, tcount, width)

    return jax.shard_map(
        body,
        mesh=mesh,
        in_specs=(
            P(None, ("gx", "gy"), None),
            P(("gx", "gy"), None, None, None),
            P(("gx", "gy"), None, None, None),
            P(),
            P(("gx", "gy"), None, None),
        ),
        out_specs=P(("gx", "gy"), None, None),
        check_vma=False,
    )
```

```python
import functools
import math

import jax
import jax.numpy as jnp
from jax import lax
from jax.experimental import pallas as pl
from jax.experimental.pallas import tpu as pltpu
from jax.sharding import PartitionSpec as P

MESH = pl.DeviceIdType.MESH
CHUNKS = 4
EARLY = 0.0


def ORDER(i, nx, ny):
    return i // ny, lax.rem(i, ny)


def split2(x):
    hi = x.astype(jnp.bfloat16)
    return hi, (x - hi.astype(jnp.float32)).astype(jnp.bfloat16)


def pool(weights, values):
    hi, lo = split2(values)
    return jnp.dot(weights, hi, preferred_element_type=jnp.float32) + jnp.dot(
        weights, lo, preferred_element_type=jnp.float32
    )


def kernel(nx, ny, tables_ref, rows_hbm, bags_hbm, hot_rows_hbm, hot_ids_hbm, out_ref,
           tab, rows_ref, bags_ref, hot_rows_ref, hot_ids_ref,
           idx_out, idx_s, stage, recv, hot_stage, hot_in, hot_part, hot_z, hot_tab,
           onehot, counts, tab_sem, in_sem, idx_send, idx_recv, idx_local, cold_send, cold_recv,
           hot_send, hot_recv, z_send, z_recv, gat_send, gat_recv):
    peers = nx * ny
    half = nx // 2
    tcount, rows_dev, width = tab.shape
    cap = rows_ref.shape[1]
    hot = hot_rows_ref.shape[1]
    chunk = hot_tab.shape[0] // ny
    batch = out_ref.shape[0]
    gx, gy = lax.axis_index("gx"), lax.axis_index("gy")
    me = gx * ny + gy

    def peer(i):
        m, j = ORDER(i, nx, ny)
        px = lax.rem(gx // half + 1 + m // half, 2) * half + lax.rem(gx + m, half)
        py = lax.rem(gy + j, ny)
        return px, py, px * ny + py

    def others(fn):
        def step(i, carry):
            px, py, p = peer(i)

            @pl.when(p != me)
            def _():
                fn(px, py, p)
            return carry
        lax.fori_loop(0, peers, step, 0)

    def plane_others(fn):
        def step(j, carry):
            fn(lax.rem(gy + j, ny))
            return carry
        lax.fori_loop(1, ny, step, 0)

    small = []
    for n, (src, dst) in enumerate(((rows_hbm, rows_ref), (hot_rows_hbm, hot_rows_ref),
                                    (bags_hbm, bags_ref), (hot_ids_hbm, hot_ids_ref))):
        load = pltpu.make_async_copy(src, dst, in_sem.at[n])
        load.start()
        small.append(load)

    piece = rows_dev // CHUNKS
    loads = []
    for t in range(tcount):
        for c in range(CHUNKS):
            part = pl.ds(c * piece, piece)
            load = pltpu.make_async_copy(tables_ref.at[t, part], tab.at[t, part], tab_sem.at[t, c])
            load.start()
            loads.append(load)

    barrier = pltpu.get_barrier_semaphore()
    others(lambda px, py, p: pl.semaphore_signal(
        barrier, inc=1, device_id=(px, py), device_id_type=MESH))

    small[0].wait()
    lines = rows_ref[...].reshape(tcount * cap, peers).T
    for p in range(peers):
        idx_out[p, :, 0:tcount * cap] = lines[p:p + 1, :]
    pl.semaphore_wait(barrier, peers - 1)

    own_idx = pltpu.make_async_copy(idx_out.at[me], idx_s.at[me], idx_local)
    own_idx.start()

    def send_idx(px, py, p):
        pltpu.make_async_remote_copy(
            src_ref=idx_out.at[p], dst_ref=idx_s.at[me], send_sem=idx_send, recv_sem=idx_recv,
            device_id=(px, py), device_id_type=MESH).start()
    others(send_idx)

    small[1].wait()
    for load in loads:
        load.wait()

    base = me * rows_dev
    group = math.gcd(chunk, 16)

    def pick_hot(y):
        def rows_of(g, carry):
            start = y * chunk + g * group
            t = start // hot
            first = start - t * hot
            for j in range(group):
                local = hot_rows_ref[t, first + j] - base
                mine = jnp.logical_and(local >= 0, local < rows_dev).astype(jnp.float32)
                at = jnp.clip(local, 0, rows_dev - 1)
                hot_stage[y, pl.ds(g * group + j, 1), :] = tab[t, pl.ds(at, 1), :] * mine
            return carry
        lax.fori_loop(0, chunk // group, rows_of, 0)

    def send_hot(y):
        pltpu.make_async_remote_copy(
            src_ref=hot_stage.at[y], dst_ref=hot_in.at[gy], send_sem=hot_send, recv_sem=hot_recv,
            device_id=(gx, y), device_id_type=MESH).start()

    def hot_step(j, carry):
        pick_hot(lax.rem(gy + j, ny))

        @pl.when(j > 1)
        def _():
            send_hot(lax.rem(gy + j - 1, ny))
        return carry
    lax.fori_loop(1, ny + 1, hot_step, 0)
    hot_in[gy] = hot_stage[gy]

    some = pl.ds(0, peers - 1)
    pltpu.make_async_copy(idx_s.at[some], idx_s.at[some], idx_recv).wait()
    own_idx.wait()

    def pick(p):
        for t in range(tcount):
            for c in range(cap):
                k = t * cap + c
                stage[p, k:k + 1, :] = tab[t, pl.ds(idx_s[p, 0, k], 1), :]

    def send_cold(i):
        px, py, p = peer(i)

        @pl.when(p != me)
        def _():
            pltpu.make_async_remote_copy(
                src_ref=stage.at[p], dst_ref=recv.at[me], send_sem=cold_send, recv_sem=cold_recv,
                device_id=(px, py), device_id_type=MESH).start()

    def cold_steps(first, last):
        def step(i, carry):
            pick(peer(i)[2])

            @pl.when(i > 0)
            def _():
                send_cold(i - 1)
            return carry
        lax.fori_loop(first, last, step, 0)

    early = int(peers * EARLY)
    cold_steps(0, early)

    planes = pl.ds(0, ny - 1)
    pltpu.make_async_copy(hot_in.at[planes], hot_in.at[planes], hot_recv).wait()
    hot_part[...] = jnp.sum(hot_in[...], axis=0)
    hot_z[gx] = hot_part[...]
    cold_steps(early, early + 1)

    def send_z(k, carry):
        pltpu.make_async_remote_copy(
            src_ref=hot_part, dst_ref=hot_z.at[gx], send_sem=z_send, recv_sem=z_recv,
            device_id=(lax.rem(gx + k, nx), gy), device_id_type=MESH).start()
        return carry
    lax.fori_loop(1, nx, send_z, 0)
    cold_steps(early + 1, peers)
    recv[me] = stage[me]
    small[2].wait()
    small[3].wait()
    send_cold(peers - 1)

    slots = peers * cap
    owner = lax.broadcasted_iota(jnp.int32, (peers, slots), 1) // cap
    spread = (owner == lax.broadcasted_iota(jnp.int32, (peers, slots), 0)).astype(jnp.float32)
    place = lax.rem(lax.broadcasted_iota(jnp.int32, (cap, slots), 1), cap)
    mask = place == lax.broadcasted_iota(jnp.int32, (cap, slots), 0)
    samples = lax.broadcasted_iota(jnp.int32, (batch, slots), 0).astype(jnp.float32)

    def cold_weights(t):
        wide = jnp.dot(bags_ref[t].astype(jnp.float32), spread,
                       precision=lax.Precision.HIGHEST, preferred_element_type=jnp.float32)
        flat = jnp.sum(jnp.where(mask, wide, 0.0), axis=0, keepdims=True)
        onehot[t] = (flat == samples).astype(jnp.bfloat16)

    cold_weights(0)

    zs = pl.ds(0, nx - 1)
    pltpu.make_async_copy(hot_z.at[zs], hot_z.at[zs], z_recv).wait()
    mine_at = pl.ds(pl.multiple_of(gy * chunk, chunk), chunk)
    hot_tab[mine_at, :] = jnp.sum(hot_z[...], axis=0)
    for t in range(1, tcount):
        cold_weights(t)

    def send_gat(y):
        pltpu.make_async_remote_copy(
            src_ref=hot_tab.at[mine_at], dst_ref=hot_tab.at[mine_at], send_sem=gat_send,
            recv_sem=gat_recv, device_id=(gx, y), device_id_type=MESH).start()
    plane_others(send_gat)

    entry = lax.broadcasted_iota(jnp.int32, (hot, batch), 0)
    for t in range(tcount):
        total = jnp.zeros((hot, batch), jnp.float32)
        for k in range(hot_ids_ref.shape[1]):
            total += (hot_ids_ref[t, k:k + 1, :] == entry).astype(jnp.float32)
        counts[t] = total.T.astype(jnp.bfloat16)

    rest = pl.ds(0, (ny - 1) * chunk)

    def pool_cold():
        pltpu.make_async_copy(recv.at[some], recv.at[some], cold_recv).wait()
        return [pool(onehot[t], recv[:, t * cap:(t + 1) * cap, :].reshape(slots, width))
                for t in range(tcount)]

    def pool_hot():
        pltpu.make_async_copy(hot_tab.at[rest], hot_tab.at[rest], gat_recv).wait()
        return [pool(counts[t], hot_tab[t * hot:(t + 1) * hot, :]) for t in range(tcount)]

    for t, part in enumerate(pool_cold()):
        out_ref[:, t * width:(t + 1) * width] = part
    for t, part in enumerate(pool_hot()):
        out_ref[:, t * width:(t + 1) * width] += part

    pltpu.make_async_copy(idx_out.at[some], idx_out.at[some], idx_send).wait()
    pltpu.make_async_copy(hot_stage.at[planes], hot_stage.at[planes], hot_send).wait()
    pltpu.make_async_copy(stage.at[some], stage.at[some], cold_send).wait()
    pltpu.make_async_copy(hot_z.at[zs], hot_z.at[zs], z_send).wait()
    pltpu.make_async_copy(hot_tab.at[rest], hot_tab.at[rest], gat_send).wait()


def solution(mesh):
    nx, ny = mesh.shape["gx"], mesh.shape["gy"]
    peers = nx * ny

    def body(tables, cold_rows, cold_bags, hot_rows, hot_ids):
        tcount, rows_dev, width = tables.shape
        cap = cold_rows.shape[3]
        batch = hot_ids.shape[0]
        hot = hot_rows.shape[1]
        chunk = tcount * hot // ny
        assert nx % 2 == 0 and chunk * ny == tcount * hot and hot % math.gcd(chunk, 16) == 0
        lanes = -(-tcount * cap // 128) * 128
        rows_t = jnp.transpose(cold_rows[0], (0, 2, 1))
        bags_t = jnp.transpose(cold_bags[0], (0, 2, 1))
        ids_t = jnp.transpose(hot_ids, (1, 2, 0))
        hbm = pl.BlockSpec(memory_space=pltpu.HBM)
        out = pl.pallas_call(
            functools.partial(kernel, nx, ny),
            out_shape=jax.ShapeDtypeStruct((batch, tcount * width), jnp.float32),
            in_specs=[hbm] * 5,
            out_specs=pl.BlockSpec(memory_space=pltpu.VMEM),
            scratch_shapes=[
                pltpu.VMEM((tcount, rows_dev, width), jnp.float32),
                pltpu.VMEM(rows_t.shape, jnp.int32),
                pltpu.VMEM(bags_t.shape, jnp.int32),
                pltpu.SMEM(hot_rows.shape, jnp.int32),
                pltpu.VMEM(ids_t.shape, jnp.int32),
                pltpu.VMEM((peers, 1, lanes), jnp.int32),
                pltpu.SMEM((peers, 1, lanes), jnp.int32),
                pltpu.VMEM((peers, tcount * cap, width), jnp.float32),
                pltpu.VMEM((peers, tcount * cap, width), jnp.float32),
                pltpu.VMEM((ny, chunk, width), jnp.float32),
                pltpu.VMEM((ny, chunk, width), jnp.float32),
                pltpu.VMEM((chunk, width), jnp.float32),
                pltpu.VMEM((nx, chunk, width), jnp.float32),
                pltpu.VMEM((tcount * hot, width), jnp.float32),
                pltpu.VMEM((tcount, batch, peers * cap), jnp.bfloat16),
                pltpu.VMEM((tcount, batch, hot), jnp.bfloat16),
                pltpu.SemaphoreType.DMA((tcount, CHUNKS)),
                pltpu.SemaphoreType.DMA((4,)),
            ] + [pltpu.SemaphoreType.DMA] * 11,
            compiler_params=pltpu.CompilerParams(
                collective_id=0, has_side_effects=True, vmem_limit_bytes=67043328),
        )(tables, rows_t, bags_t, hot_rows, ids_t)
        return out.reshape(batch, tcount, width)

    return jax.shard_map(
        body,
        mesh=mesh,
        in_specs=(
            P(None, ("gx", "gy"), None),
            P(("gx", "gy"), None, None, None),
            P(("gx", "gy"), None, None, None),
            P(),
            P(("gx", "gy"), None, None),
        ),
        out_specs=P(("gx", "gy"), None, None),
        check_vma=False,
    )
```
